32 devices in a mesh: corpus: 16 (over z, y, x), batch: 2 (over core).
Axes of the slice: x: 2, y: 2, z: 4, core: 2. Of those that a mesh axis runs over, the one named last changes fastest.
Arguments:
- queries: float32 [128, 1024], P(('corpus', 'batch')), may hold values from -6.25 to 6.25, as said below
- codes: int32 [98304, 32], P('corpus'), may hold values from -2147483648 to 2147483647
- quant_rows: bfloat16 [98304, 1024], P('corpus'), may hold values from -127 to 127, as said below
- row_scale: float32 [98304], P('corpus'), may hold values from 0.0005 to 0.002
- candidates: int32 [128, 40], P(('corpus', 'batch')), may hold values from 0 to 98303
- shortlist: int32 [128], P(('corpus', 'batch')), may hold values from 1 to 40
- edges: int32 [17], replicated, may hold values from 464 to 563, as said below
Outputs:
- hist: float32 [128, 16], P(('corpus', 'batch'))
- scores: float32 [128, 40], P(('corpus', 'batch'))
The draws below stay inside these ranges and needn't reach their ends.
Inputs may be any that keep to these rules, and one draw needn't show every extreme that they name: `queries`: no entry lies within 0.25 of zero. `quant_rows`: whole numbers. `edges`: strictly increasing.
All inputs are finite; a program needn't handle non-finite values.
Results may differ from the reference program's by a relative error of at most 0.0003.
Values sent between devices are 32-bit elements; how exact they have to be, the bound alone decides.
A program may use at most 64 MiB of HBM per device.

```python
import math
import jax
import jax.numpy as jnp
import numpy as np
from jax import lax

D = 1024
WORDS = 32
QUERIES = 128
ROWS_DEV = 6144
TOTAL_ROWS = 98304
CAND = 40
NBINS = 16
N_CORPUS = 16


def centers(key):
    return jax.random.randint(jax.random.fold_in(key, 101), (16, D), 0, 2).astype(jnp.int32)


def draw_queries(key, part):
    pattern = centers(key)
    member = jax.random.randint(jax.random.fold_in(key, 102), (QUERIES,), 0, 16)
    flip_level = jax.random.randint(jax.random.fold_in(key, 103), (QUERIES, 1), 0, 48)
    flipped = (jax.random.randint(jax.random.fold_in(key, 104), (QUERIES, D), 0, 1024) < flip_level).astype(jnp.int32)
    bits = jnp.bitwise_xor(pattern[member], flipped)
    sign = (2 * bits - 1).astype(jnp.float32)
    normal_part = jax.random.normal(jax.random.fold_in(key, 105), (QUERIES, D), jnp.float32)
    magnitude = 0.25 + jnp.minimum(jnp.abs(normal_part), 6.0)
    return sign * magnitude


def draw_codes(key, part):
    groups = 16
    pattern = centers(key)
    region = jnp.arange(TOTAL_ROWS, dtype=jnp.int32) * groups // TOTAL_ROWS
    member = (region + jax.random.randint(jax.random.fold_in(key, 106), (TOTAL_ROWS,), 0, 2)) % groups
    factor = max(1, 32 // math.isqrt(D))
    level = 512 - jax.random.randint(jax.random.fold_in(key, 107), (groups,), 12, 37) * factor
    chance = level[member] + jax.random.randint(jax.random.fold_in(key, 108), (TOTAL_ROWS,), -16, 17) * factor
    block = math.gcd(TOTAL_ROWS, 2048)
    shifts = jnp.arange(32, dtype=jnp.int32)
    noise_key = jax.random.fold_in(key, 109)

    def one_block(number):
        start = number * block
        own = lax.dynamic_slice_in_dim(member, start, block, 0)
        odds = lax.dynamic_slice_in_dim(chance, start, block, 0)
        noise = (jax.random.randint(jax.random.fold_in(noise_key, number), (block, D), 0, 1024) < odds[:, None]).astype(jnp.int32)
        bits = jnp.bitwise_xor(pattern[own], noise).reshape(block, D // 32, 32)
        return jnp.sum(jnp.left_shift(bits, shifts), axis=2).astype(jnp.int32)
    whole = lax.map(one_block, jnp.arange(TOTAL_ROWS // block, dtype=jnp.int32))
    return whole.reshape(TOTAL_ROWS, D // 32)


def draw_quant_rows(key, part):
    whole = jax.random.randint(key, (TOTAL_ROWS, D), -127, 128)
    return whole.astype(jnp.float32).astype(jnp.bfloat16)


def draw_edges(key, part):
    spacing = max(2, 3 * D // 512)
    jitter = jax.random.randint(key, (NBINS + 1,), 0, spacing // 2 + 1)
    slots = jnp.arange(NBINS + 1, dtype=jnp.int32)
    jitter = jnp.where(slots == 0, 0, jnp.where(slots == NBINS, spacing // 2, jitter))
    start = D // 2 - spacing * (NBINS // 2)
    return (start + spacing * slots + jitter).astype(jnp.int32)


def set_ends(array, stream_key, least, high):
    extent = array.shape
    index_at = [jax.random.randint(jax.random.fold_in(stream_key, axis), (), 0, extent[axis]) for axis in range(len(extent))]
    array = array.at[tuple(index_at)].set(least)
    longest = extent.index(max(extent))
    index_at[longest] = (index_at[longest] + 1) % extent[longest]
    return array.at[tuple(index_at)].set(high)


def levels(stream_key, dims, cuts, low, largest):
    def one(position, shards_of):
        steps = jax.random.uniform(jax.random.fold_in(jax.random.fold_in(stream_key, 6), position), (shards_of,), jnp.float32, low / len(cuts), largest / len(cuts))
        return jnp.repeat(jnp.exp(steps), dims[position] // shards_of).reshape((-1,) + (1,) * (len(dims) - position - 1))

    loudness = one(*cuts[0])
    for cut in cuts[1:]:
        loudness = loudness * one(*cut)
    return loudness


def skewed_wide(key, extent, number_of, lean):
    loads = [min(1 << octave, number_of + 1 - (1 << octave)) * (1 << 20) // math.isqrt((1 << octave) ** lean) + 1 for octave in range((number_of + 1).bit_length()) if 1 << octave <= number_of]
    width = 1 + sum(loads) // (1 << 30)
    table = np.cumsum(np.array([max(1, weight // width) for weight in loads]))
    ticket = jax.random.randint(jax.random.fold_in(key, 1), extent, 0, int(table[len(loads) - 1]))
    start = jnp.left_shift(1, jnp.searchsorted(jnp.asarray(table, jnp.int32), ticket, side="right").astype(jnp.int32))
    standing = start - 1 + jax.random.randint(jax.random.fold_in(key, 4), extent, 0, 1 << 30) % jnp.minimum(start, number_of + 1 - start)
    return jax.random.permutation(jax.random.fold_in(key, 2), number_of)[standing].astype(jnp.int32)


def setup_inputs(seed: int = 0) -> dict:
    splits = jax.random.split(jax.random.key(seed), 8)
    queries = draw_queries(jax.random.fold_in(splits[7], 71), 0)
    codes = draw_codes(jax.random.fold_in(splits[7], 71), 0)
    quant_rows = draw_quant_rows(jax.random.fold_in(splits[7], 71), 0)
    row_scale = jnp.clip(jnp.exp(math.log(0.002) - 1.3862944 * jax.random.uniform(splits[3], (TOTAL_ROWS,), jnp.float32) ** levels(splits[3], (TOTAL_ROWS,), ((0, 16),), -0.2, 0.2)), 0.0005, 0.002)
    candidates = set_ends(skewed_wide(splits[4], (QUERIES, CAND), TOTAL_ROWS, 2), jax.random.fold_in(splits[4], 3), 0, TOTAL_ROWS - 1).astype(jnp.int32)
    shortlist = set_ends(jax.random.randint(splits[5], (QUERIES,), 1, CAND + 1), jax.random.fold_in(splits[5], 1), 1, CAND).astype(jnp.int32)
    edges = draw_edges(jax.random.fold_in(splits[7], 71), 0)
    return dict(queries=queries, codes=codes, quant_rows=quant_rows, row_scale=row_scale, candidates=candidates, shortlist=shortlist, edges=edges)


def unpack(words):
    bits = jnp.right_shift(words[..., None], jnp.arange(32, dtype=jnp.int32)) & 1
    signed = (2 * bits - 1).reshape(words.shape[:-1] + (words.shape[-1] * 32,))
    return signed.astype(jnp.bfloat16)


def reference(queries, codes, quant_rows, row_scale, candidates, shortlist, edges):
    signs = jnp.where(queries >= 0, 1.0, -1.0).astype(jnp.bfloat16)
    limits = edges.astype(jnp.float32)
    blocks = codes.reshape(N_CORPUS, ROWS_DEV, WORDS)

    def step(total, words):
        plus = unpack(words)
        inner = jnp.dot(signs, plus.T, preferred_element_type=jnp.float32)
        ham = (D - inner) * 0.5
        above = jnp.stack([jnp.sum((ham >= limits[k]).astype(jnp.float32), axis=1) for k in range(NBINS + 1)], axis=1)
        return total + above, None

    above, _ = lax.scan(step, jnp.zeros((QUERIES, NBINS + 1), jnp.float32), blocks)
    counts = above[:, :-1] - above[:, 1:]
    hist = counts * (NBINS / TOTAL_ROWS)
    picked = quant_rows[candidates].astype(jnp.float32)
    raw = jnp.einsum("qd,qjd->qj", queries.astype(jnp.float32), picked, precision=lax.Precision.HIGHEST)
    slots = jnp.arange(CAND, dtype=jnp.int32)
    live = slots[None, :] < shortlist[:, None]
    scores = jnp.where(live, raw * row_scale[candidates], 0.0)
    return hist, scores
```

```python
import functools

import jax
import jax.numpy as jnp
from jax import lax
from jax.experimental import pallas as pl
from jax.experimental.pallas import tpu as pltpu
from jax.sharding import PartitionSpec as P

LANES = 128
HIST_AT = 64


def grid_of(n):
    side = 1
    while 2 * side**3 < n:
        side += 1
    return (n // (side * side), side, side) if 2 * side**3 == n else (n, 1, 1)


def kernel(
    n, cores, queries, cands, lens, edges, scale, codes_hbm, quant_hbm,
    hist_out, scores_out,
    own, gathered, words, quant, plus, flat, split, signs, marks, part, part_out, part_in,
    words_sem, quant_sem, send_sem, recv_sem, out_sem, in_sem,
):
    zs, ys, xs = grid_of(n)
    chip, core = lax.axis_index("corpus"), lax.axis_index("batch")
    me = chip * cores + core
    rows_q, width = queries.shape
    total = n * cores
    span = quant.shape[0]
    count_k = edges.shape[0]
    chunk = quant.shape[0] // quant_sem.shape[0]
    first = core * span

    words_copy = pltpu.make_async_copy(
        codes_hbm.at[:, pl.ds(pl.multiple_of(first, LANES), span)], words, words_sem
    )
    words_copy.start()

    def quant_copy(i):
        at = pl.multiple_of(first + i * chunk, chunk)
        to = pl.multiple_of(i * chunk, chunk)
        return pltpu.make_async_copy(
            quant_hbm.at[pl.ds(at, chunk)], quant.at[pl.ds(to, chunk)], quant_sem.at[i]
        )

    for i in range(quant_sem.shape[0]):
        quant_copy(i).start()

    own[:, :width] = queries[...]
    row = lax.broadcasted_iota(jnp.int32, cands.shape, 0)
    slot = lax.broadcasted_iota(jnp.int32, cands.shape, 1)
    length = jnp.zeros(cands.shape, jnp.int32)
    for i in range(rows_q):
        length = jnp.where(row == i, lens[i], length)
    own[:, width:] = jnp.full((rows_q, LANES), -1.0, jnp.float32)
    own[:, width : width + cands.shape[1]] = jnp.where(
        slot < length, cands[...], -1
    ).astype(jnp.float32)

    z, y, x = chip // (ys * xs), (chip // xs) % ys, chip % xs
    even = core % 2 == 0
    stride_b = jnp.where(even, xs, 1)
    stride_c = jnp.where(even, 1, xs)
    b, c = jnp.where(even, y, x), jnp.where(even, x, y)
    bs, cs = ys, xs

    def chip_at(zz, bb, cc):
        return zz * (ys * xs) + bb * stride_b + cc * stride_c

    barrier = pltpu.get_barrier_semaphore()
    peers = []
    for i in range(1, zs):
        peers.append((chip_at((z + i) % zs, b, c), core))
    for i in range(1, bs):
        peers.append((chip_at(z, (b + i) % bs, c), core))
    for i in range(1, cs):
        peers.append((chip_at(z, b, (c + i) % cs), core))
    for i in range(1, cores):
        peers.append((chip, (core + i) % cores))
    for to in peers:
        pl.semaphore_signal(barrier, inc=1, device_id=to, device_id_type=pl.DeviceIdType.MESH)
    pl.semaphore_wait(barrier, len(peers))
    n_peers = len(peers)
    to_z, to_b = zs - 1, bs - 1
    to_c = cs - 1

    def block_copy(block, kind, to, mine=False):
        return pltpu.make_async_remote_copy(
            src_ref=own if mine else gathered.at[block],
            dst_ref=gathered.at[block],
            send_sem=send_sem.at[kind],
            recv_sem=recv_sem.at[block],
            device_id=to,
            device_id_type=pl.DeviceIdType.MESH,
        )

    def got(block):
        pltpu.make_async_copy(gathered.at[block], gathered.at[block], recv_sem.at[block]).wait()

    def pass_on(block, lo, mine=False):
        for kind in range(lo, n_peers):
            block_copy(block, kind, peers[kind], mine).start()

    def block_z(i):
        return chip_at((z + i) % zs, b, c) * cores + core

    def block_b(i):
        return chip_at((z + i % zs) % zs, (b + 1 + i // zs) % bs, c) * cores + core

    def block_c(i):
        return (
            chip_at((z + i % zs) % zs, (b + (i // zs) % bs) % bs, (c + 1 + i // (zs * bs)) % cs) * cores
            + core
        )

    def block_d(i):
        return (i % n) * cores + (core + 1 + i // n) % cores

    def sent():
        counts = [1] * to_z + [zs] * to_b + [zs * bs] * to_c + [n] * (cores - 1)
        for kind, count in enumerate(counts):
            some = gathered.at[pl.ds(0, count)]
            pltpu.make_async_copy(some, some, send_sem.at[kind]).wait()

    count_b, count_c, count_d = zs * to_b, zs * bs * to_c, n * (cores - 1)
    at_b, at_c, at_d = to_z, to_z + to_b, to_z + to_b + to_c

    def loop(lo, hi, body):
        def step(i, carry):
            body(i)
            return carry

        lax.fori_loop(lo, hi, step, 0)

    bit = lax.broadcasted_iota(jnp.int32, (32, span // 2), 0)

    def unpack(lo, hi):
        def step(w):
            for half in range(2):
                cols = slice(half * (span // 2), (half + 1) * (span // 2))
                word = jnp.broadcast_to(words[pl.ds(w, 1), cols], bit.shape)
                bits = jnp.bitwise_and(lax.shift_right_logical(word, bit), 1)
                plus[pl.ds(pl.multiple_of(w * 32, 32), 32), cols] = bits.astype(
                    jnp.float32
                ).astype(jnp.bfloat16)

        loop(lo, hi, step)

    count_w = words.shape[0]
    cut = [count_w * i // 4 for i in range(5)]

    pass_on(me, 0, True)
    gathered[me] = own[...]
    words_copy.wait()
    unpack(cut[0], cut[1])

    def relay(block_of, lo, start=0):
        def step(i):
            block = block_of(i)
            got(block)
            pass_on(block, lo)

        return step

    loop(1, zs, relay(block_z, at_b))
    unpack(cut[1], cut[2])
    loop(0, count_b, relay(block_b, at_c))
    unpack(cut[2], cut[3])
    loop(0, count_c, relay(block_c, at_d))
    unpack(cut[3], cut[4])
    loop(0, count_d, lambda i: got(block_d(i)))

    def lay(i):
        pair = jnp.concatenate([gathered[2 * i], gathered[2 * i + 1]], axis=0)
        flat[pl.ds(pl.multiple_of(i * 2 * rows_q, 2 * rows_q), 2 * rows_q), :] = pair

    loop(0, total // 2, lay)
    for i in range(quant_sem.shape[0]):
        quant_copy(i).wait()

    tile_q = marks.shape[1]
    groups = span // chunk
    base = (chip * cores + core) * span
    limits = [(edges[k] - width // 2).astype(jnp.float32).astype(jnp.bfloat16) for k in range(count_k)]

    def tile(t):
        q_at = pl.multiple_of(t * tile_q, tile_q)
        vecs = flat[pl.ds(q_at, tile_q), :width]
        index = flat[pl.ds(q_at, tile_q), width:].astype(jnp.int32) - base
        high = vecs.astype(jnp.bfloat16)
        split[:tile_q] = high
        split[tile_q:] = (vecs - high.astype(jnp.float32)).astype(jnp.bfloat16)
        sign = jnp.where(vecs >= 0, 1.0, -1.0)
        signs[...] = sign.astype(jnp.bfloat16)
        half_sum = jnp.sum(sign, axis=1, keepdims=True) * 0.5
        lane = jnp.bitwise_and(index, LANES - 1)
        where = lax.shift_right_arithmetic(index, 7)
        marks[...] = jnp.zeros_like(marks)
        part[...] = jnp.zeros_like(part)

        def step(g):
            r_at = pl.multiple_of(g * chunk, chunk)
            dots = jnp.dot(signs[...], plus[:, pl.ds(r_at, chunk)], preferred_element_type=jnp.float32)
            ham = (half_sum - dots).astype(jnp.bfloat16)
            one = jnp.ones((tile_q, LANES), jnp.bfloat16)
            for k in range(count_k):
                mark = marks[k]
                for j in range(chunk // LANES):
                    piece = ham[:, j * LANES : (j + 1) * LANES]
                    mark = mark + jnp.where(piece >= limits[k], one, jnp.zeros_like(one))
                marks[k] = mark
            both = lax.dot_general(
                split[...], quant[pl.ds(r_at, chunk), :], (((1,), (1,)), ((), ())),
                preferred_element_type=jnp.float32,
            )
            raw = both[:tile_q] + both[tile_q:]
            score = part[...]
            for j in range(chunk // LANES):
                row_at = core * (span // LANES) + g * (chunk // LANES) + j
                piece = raw[:, j * LANES : (j + 1) * LANES] * scale[pl.ds(row_at, 1), :]
                picked = jnp.take_along_axis(piece, lane, axis=1, mode="promise_in_bounds")
                score = jnp.where(where == g * (chunk // LANES) + j, picked, score)
            part[...] = score

        loop(0, groups, step)
        columns = lax.broadcasted_iota(jnp.int32, (LANES, LANES), 1)
        result = part[...]
        for k in range(count_k):
            spot = jnp.where(columns == HIST_AT + k, 1.0, 0.0).astype(jnp.bfloat16)
            result = result + jnp.dot(marks[k], spot, preferred_element_type=jnp.float32)
        per = tile_q // rows_q
        for i in range(per):
            part_out[t * per + i] = result[i * rows_q : (i + 1) * rows_q]

    loop(0, flat.shape[0] // tile_q, tile)

    def result_copy(i):
        to = (me + i) % total
        return pltpu.make_async_remote_copy(
            src_ref=part_out.at[to],
            dst_ref=part_in.at[me],
            send_sem=out_sem,
            recv_sem=in_sem.at[me],
            device_id=(to // cores, to % cores),
            device_id_type=pl.DeviceIdType.MESH,
        )

    loop(1, total, lambda i: result_copy(i).start())
    part_in[me] = part_out[me]

    def wait_in(i):
        source = (me + i) % total
        pltpu.make_async_copy(part_in.at[source], part_in.at[source], in_sem.at[source]).wait()

    loop(1, total, wait_in)
    summed = jnp.sum(part_in[...], axis=0)
    bins = count_k - 1
    above = summed[:, HIST_AT : HIST_AT + bins] - summed[:, HIST_AT + 1 : HIST_AT + 1 + bins]
    hist_out[...] = above * (bins / (total * span))
    scores_out[...] = summed[:, : cands.shape[1]]

    rest = part_in.at[pl.ds(0, total - 1)]
    pltpu.make_async_copy(rest, rest, out_sem).wait()
    sent()


def shards(n, cores, queries, codes, quant_rows, row_scale, candidates, shortlist, edges):
    rows_q, width = queries.shape
    count_rows, count_w = codes.shape
    span = count_rows // cores
    total = n * cores
    tile_q = 128
    chunk = 512
    vmem, smem, hbm = pltpu.VMEM, pltpu.SMEM, pl.ANY
    zs, ys, xs = grid_of(n)
    n_peers = zs + ys + xs + cores - 4
    f32, bf16 = jnp.float32, jnp.bfloat16
    spec = pl.BlockSpec
    return pl.pallas_call(
        functools.partial(kernel, n, cores),
        out_shape=(
            jax.ShapeDtypeStruct((rows_q, edges.shape[0] - 1), f32),
            jax.ShapeDtypeStruct(candidates.shape, f32),
        ),
        in_specs=[
            spec(memory_space=vmem), spec(memory_space=vmem), spec(memory_space=smem),
            spec(memory_space=smem), spec(memory_space=vmem), spec(memory_space=hbm),
            spec(memory_space=hbm),
        ],
        out_specs=(spec(memory_space=vmem), spec(memory_space=vmem)),
        scratch_shapes=[
            vmem((rows_q, width + LANES), f32),
            vmem((total, rows_q, width + LANES), f32),
            vmem((count_w, span), jnp.int32),
            vmem((span, width), bf16),
            vmem((width, span), bf16),
            vmem((total * rows_q, width + LANES), f32),
            vmem((2 * tile_q, width), bf16),
            vmem((tile_q, width), bf16),
            vmem((edges.shape[0], tile_q, LANES), bf16),
            vmem((tile_q, LANES), f32),
            vmem((total, rows_q, LANES), f32),
            vmem((total, rows_q, LANES), f32),
            pltpu.SemaphoreType.DMA,
            pltpu.SemaphoreType.DMA((span // chunk,)),
            pltpu.SemaphoreType.DMA((n_peers,)),
            pltpu.SemaphoreType.DMA((total,)),
            pltpu.SemaphoreType.DMA,
            pltpu.SemaphoreType.DMA((total,)),
        ],
        compiler_params=pltpu.CompilerParams(
            collective_id=0, has_side_effects=True, vmem_limit_bytes=60 * 1024 * 1024
        ),
        name="search",
    )(
        queries, candidates, shortlist, edges,
        row_scale.reshape(count_rows // LANES, LANES), codes.T, quant_rows,
    )


def solution(mesh):
    return jax.shard_map(
        functools.partial(shards, mesh.shape["corpus"], mesh.shape["batch"]),
        mesh=mesh,
        in_specs=(
            P(("corpus", "batch"), None),
            P("corpus", None),
            P("corpus", None),
            P("corpus"),
            P(("corpus", "batch"), None),
            P(("corpus", "batch")),
            P(),
        ),
        out_specs=(P(("corpus", "batch"), None), P(("corpus", "batch"), None)),
        check_vma=False,
    )
```

```python
import functools

import jax
import jax.numpy as jnp
from jax import lax
from jax.experimental import pallas as pl
from jax.experimental.pallas import tpu as pltpu
from jax.sharding import PartitionSpec as P

LANES = 128
HIST_AT = 64


def grid_of(n):
    side = 1
    while 2 * side**3 < n:
        side += 1
    return (n // (side * side), side, side) if 2 * side**3 == n else (n, 1, 1)


def kernel(
    n, cores, queries_hbm, cands_hbm, lens_hbm, edges_hbm, scale_hbm, codes_hbm, quant_hbm,
    out,
    queries, cands, lens, edges, scale, own, gathered, words, quant, plus, flat, split, signs, marks, part, ham_a, ham_b, raw_a, raw_b, part_out, part_in,
    small_sem, words_sem, quant_sem, send_sem, recv_sem, out_sem, in_sem,
):
    zs, ys, xs = grid_of(n)
    chip, core = lax.axis_index("corpus"), lax.axis_index("batch")
    me = chip * cores + core
    rows_q, width = queries.shape
    total = n * cores
    span = quant.shape[0]
    count_k = edges.shape[0]
    chunk = quant.shape[0] // quant_sem.shape[0]
    first = core * span

    z, y, x = chip // (ys * xs), (chip // xs) % ys, chip % xs
    even = core % 2 == 0
    stride_b = jnp.where(even, xs, 1)
    stride_c = jnp.where(even, 1, xs)
    b, c = jnp.where(even, y, x), jnp.where(even, x, y)
    bs, cs = ys, xs

    def chip_at(zz, bb, cc):
        return zz * (ys * xs) + bb * stride_b + cc * stride_c

    barrier = pltpu.get_barrier_semaphore()
    peers = []
    for i in range(1, zs):
        peers.append((chip_at((z + i) % zs, b, c), core))
    for i in range(1, bs):
        peers.append((chip_at(z, (b + i) % bs, c), core))
    for i in range(1, cs):
        peers.append((chip_at(z, b, (c + i) % cs), core))
    for i in range(1, cores):
        peers.append((chip, (core + i) % cores))
    for to in peers:
        pl.semaphore_signal(barrier, inc=1, device_id=to, device_id_type=pl.DeviceIdType.MESH)
    smalls = [
        pltpu.make_async_copy(source, target, small_sem.at[i])
        for i, (source, target) in enumerate(
            (
                (queries_hbm, queries), (cands_hbm, cands), (lens_hbm, lens),
                (edges_hbm, edges), (scale_hbm, scale),
            )
        )
    ]
    for copy in smalls:
        copy.start()

    words_copy = pltpu.make_async_copy(
        codes_hbm.at[:, pl.ds(pl.multiple_of(first, LANES), span)], words, words_sem
    )
    words_copy.start()

    def quant_copy(i):
        at = pl.multiple_of(first + i * chunk, chunk)
        to = pl.multiple_of(i * chunk, chunk)
        return pltpu.make_async_copy(
            quant_hbm.at[pl.ds(at, chunk)], quant.at[pl.ds(to, chunk)], quant_sem.at[i]
        )

    for i in range(quant_sem.shape[0]):
        quant_copy(i).start()

    for copy in smalls:
        copy.wait()

    own[:, :width] = queries[...]
    row = lax.broadcasted_iota(jnp.int32, cands.shape, 0)
    slot = lax.broadcasted_iota(jnp.int32, cands.shape, 1)
    length = jnp.zeros(cands.shape, jnp.int32)
    for i in range(rows_q):
        length = jnp.where(row == i, lens[i], length)
    own[:, width:] = jnp.full((rows_q, LANES), -1.0, jnp.float32)
    own[:, width : width + cands.shape[1]] = jnp.where(
        slot < length, cands[...], -1
    ).astype(jnp.float32)

    pl.semaphore_wait(barrier, len(peers))
    n_peers = len(peers)
    to_z, to_b = zs - 1, bs - 1
    to_c = cs - 1

    def block_copy(block, kind, to, mine=False):
        return pltpu.make_async_remote_copy(
            src_ref=own if mine else gathered.at[block],
            dst_ref=gathered.at[block],
            send_sem=send_sem.at[kind],
            recv_sem=recv_sem.at[block],
            device_id=to,
            device_id_type=pl.DeviceIdType.MESH,
        )

    def got(block):
        pltpu.make_async_copy(gathered.at[block], gathered.at[block], recv_sem.at[block]).wait()

    def pass_on(block, lo, mine=False):
        for kind in range(lo, n_peers):
            block_copy(block, kind, peers[kind], mine).start()

    both_sides = jnp.minimum(z, zs - 1 - z)
    far_side = jnp.where(z < zs - 1 - z, 1, -1)

    def z_at(p):
        near = p <= 2 * both_sides
        away = jnp.where(near, (p + 1) // 2, p - both_sides)
        side = jnp.where(near, 2 * (p % 2) - 1, far_side)
        return z + away * side

    def block_z(p):
        return chip_at(z_at(p), b, c) * cores + core

    def block_b(i):
        return chip_at(z_at(i % zs), (b + 1 + i // zs) % bs, c) * cores + core

    def block_c(i):
        to = (c + 1 + i // (zs * bs)) % cs
        return chip_at(z_at(i % zs), (b + (i // zs) % bs) % bs, to) * cores + core

    def block_d(i):
        return (i % n) * cores + (core + 1 + i // n) % cores

    def sent():
        counts = [1] * to_z + [zs] * to_b + [zs * bs] * to_c + [n] * (cores - 1)
        for kind, count in enumerate(counts):
            some = gathered.at[pl.ds(0, count)]
            pltpu.make_async_copy(some, some, send_sem.at[kind]).wait()

    count_b, count_c, count_d = zs * to_b, zs * bs * to_c, n * (cores - 1)
    at_b, at_c, at_d = to_z, to_z + to_b, to_z + to_b + to_c

    def loop(lo, hi, body):
        def step(i, carry):
            body(i)
            return carry

        lax.fori_loop(lo, hi, step, 0)

    bit = lax.broadcasted_iota(jnp.int32, (32, span // 2), 0)

    def unpack(lo, hi):
        def step(w):
            for half in range(2):
                cols = slice(half * (span // 2), (half + 1) * (span // 2))
                word = jnp.broadcast_to(words[pl.ds(w, 1), cols], bit.shape)
                bits = jnp.bitwise_and(lax.shift_right_logical(word, bit), 1)
                plus[pl.ds(pl.multiple_of(w * 32, 32), 32), cols] = bits.astype(
                    jnp.float32
                ).astype(jnp.bfloat16)

        loop(lo, hi, step)

    count_w = words.shape[0]
    cut = [count_w * i // 4 for i in range(5)]

    pass_on(me, 0, True)
    gathered[me] = own[...]
    words_copy.wait()
    unpack(cut[0], cut[1])

    def relay(block_of, lo, start=0):
        def step(i):
            block = block_of(i)
            got(block)
            pass_on(block, lo)

        return step

    loop(1, min(2, zs), relay(block_z, at_b))
    loop(0, to_b, lambda i: relay(block_b, at_c)(i * zs))
    loop(min(2, zs), zs, relay(block_z, at_b))
    unpack(cut[1], cut[2])
    loop(0, to_b * (zs - 1), lambda i: relay(block_b, at_c)(i // (zs - 1) * zs + 1 + i % (zs - 1)))
    unpack(cut[2], cut[3])
    loop(0, count_c, relay(block_c, at_d))
    unpack(cut[3], cut[4])
    loop(0, count_d, lambda i: got(block_d(i)))

    def lay(i):
        pair = jnp.concatenate([gathered[2 * i], gathered[2 * i + 1]], axis=0)
        flat[pl.ds(pl.multiple_of(i * 2 * rows_q, 2 * rows_q), 2 * rows_q), :] = pair

    loop(0, total // 2, lay)
    for i in range(quant_sem.shape[0]):
        quant_copy(i).wait()

    tile_q = marks.shape[1]
    unit = ham_a.shape[1]
    groups = span // unit
    base = (chip * cores + core) * span
    limits = [(edges[k] - width // 2).astype(jnp.float32).astype(jnp.bfloat16) for k in range(count_k)]

    def tile(t):
        q_at = pl.multiple_of(t * tile_q, tile_q)
        vecs = flat[pl.ds(q_at, tile_q), :width]
        index = flat[pl.ds(q_at, tile_q), width:].astype(jnp.int32) - base
        high = vecs.astype(jnp.bfloat16)
        split[:tile_q] = high
        split[tile_q:] = (vecs - high.astype(jnp.float32)).astype(jnp.bfloat16)
        sign = jnp.where(vecs >= 0, 1.0, -1.0)
        signs[...] = sign.astype(jnp.bfloat16)
        half_sum = jnp.sum(sign, axis=1, keepdims=True) * 0.5
        lane = jnp.bitwise_and(index, LANES - 1)
        where = lax.shift_right_arithmetic(index, 7)
        marks[...] = jnp.zeros_like(marks)
        part[...] = jnp.zeros_like(part)

        def multiply(g, ham, raw):
            r_at = pl.multiple_of(g * unit, unit)
            dots = jnp.dot(signs[...], plus[:, pl.ds(r_at, unit)], preferred_element_type=jnp.float32)
            ham[...] = (half_sum - dots).astype(jnp.bfloat16)
            both = lax.dot_general(
                split[...], quant[pl.ds(r_at, unit), :], (((1,), (1,)), ((), ())),
                preferred_element_type=jnp.float32,
            )
            raw[...] = both[:tile_q] + both[tile_q:]

        def collect(g, ham, raw):
            one = jnp.ones((tile_q, LANES), jnp.bfloat16)
            for k in range(count_k):
                mark = marks[k]
                for j in range(unit // LANES):
                    piece = ham[:, j * LANES : (j + 1) * LANES]
                    mark = mark + jnp.where(piece >= limits[k], one, jnp.zeros_like(one))
                marks[k] = mark
            score = part[...]
            for j in range(unit // LANES):
                row_at = core * (span // LANES) + g * (unit // LANES) + j
                piece = raw[:, j * LANES : (j + 1) * LANES] * scale[pl.ds(row_at, 1), :]
                picked = jnp.take_along_axis(piece, lane, axis=1, mode="promise_in_bounds")
                score = jnp.where(where == g * (unit // LANES) + j, picked, score)
            part[...] = score

        def step(p):
            multiply(2 * p + 1, ham_b, raw_b)
            collect(2 * p, ham_a, raw_a)
            multiply(2 * p + 2, ham_a, raw_a)
            collect(2 * p + 1, ham_b, raw_b)

        multiply(0, ham_a, raw_a)
        loop(0, groups // 2 - 1, step)
        multiply(groups - 1, ham_b, raw_b)
        collect(groups - 2, ham_a, raw_a)
        collect(groups - 1, ham_b, raw_b)
        columns = lax.broadcasted_iota(jnp.int32, (LANES, LANES), 1)
        result = part[...]
        for k in range(count_k):
            spot = jnp.where(columns == HIST_AT + k, 1.0, 0.0).astype(jnp.bfloat16)
            result = result + jnp.dot(marks[k], spot, preferred_element_type=jnp.float32)
        per = tile_q // rows_q
        for i in range(per):
            part_out[t * per + i] = result[i * rows_q : (i + 1) * rows_q]

    loop(0, flat.shape[0] // tile_q, tile)

    def result_copy(i):
        to = (me + i) % total
        return pltpu.make_async_remote_copy(
            src_ref=part_out.at[to],
            dst_ref=part_in.at[me],
            send_sem=out_sem,
            recv_sem=in_sem.at[me],
            device_id=(to // cores, to % cores),
            device_id_type=pl.DeviceIdType.MESH,
        )

    loop(1, total, lambda i: result_copy(i).start())
    part_in[me] = part_out[me]

    def wait_in(i):
        source = (me + i) % total
        pltpu.make_async_copy(part_in.at[source], part_in.at[source], in_sem.at[source]).wait()

    loop(1, total, wait_in)
    summed = jnp.sum(part_in[...], axis=0)
    bins = count_k - 1
    above = summed[:, HIST_AT : HIST_AT + bins] - summed[:, HIST_AT + 1 : HIST_AT + 1 + bins]
    out[:, HIST_AT : HIST_AT + bins] = above * (bins / (total * span))
    out[:, : cands.shape[1]] = summed[:, : cands.shape[1]]

    rest = part_in.at[pl.ds(0, total - 1)]
    pltpu.make_async_copy(rest, rest, out_sem).wait()
    sent()


def finish(rows, hist, scores):
    hist[...] = rows[:, HIST_AT : HIST_AT + hist.shape[1]]
    scores[...] = rows[:, : scores.shape[1]]


def shards(n, cores, queries, codes, quant_rows, row_scale, candidates, shortlist, edges):
    rows_q, width = queries.shape
    count_rows, count_w = codes.shape
    span = count_rows // cores
    total = n * cores
    tile_q = 128
    chunk = 512
    unit = 512
    vmem, smem, hbm = pltpu.VMEM, pltpu.SMEM, pl.ANY
    zs, ys, xs = grid_of(n)
    n_peers = zs + ys + xs + cores - 4
    f32, bf16 = jnp.float32, jnp.bfloat16
    spec = pl.BlockSpec
    rows = pl.pallas_call(
        functools.partial(kernel, n, cores),
        out_shape=jax.ShapeDtypeStruct((rows_q, LANES), f32),
        in_specs=[
            spec(memory_space=hbm) for _ in range(7)
        ],
        out_specs=spec(memory_space=vmem),
        scratch_shapes=[
            vmem(queries.shape, f32),
            vmem(candidates.shape, jnp.int32),
            smem(shortlist.shape, jnp.int32),
            smem(edges.shape, jnp.int32),
            vmem((count_rows // LANES, LANES), f32),
            vmem((rows_q, width + LANES), f32),
            vmem((total, rows_q, width + LANES), f32),
            vmem((count_w, span), jnp.int32),
            vmem((span, width), bf16),
            vmem((width, span), bf16),
            vmem((total * rows_q, width + LANES), f32),
            vmem((2 * tile_q, width), bf16),
            vmem((tile_q, width), bf16),
            vmem((edges.shape[0], tile_q, LANES), bf16),
            vmem((tile_q, LANES), f32),
            vmem((tile_q, unit), bf16),
            vmem((tile_q, unit), bf16),
            vmem((tile_q, unit), f32),
            vmem((tile_q, unit), f32),
            vmem((total, rows_q, LANES), f32),
            vmem((total, rows_q, LANES), f32),
            pltpu.SemaphoreType.DMA((5,)),
            pltpu.SemaphoreType.DMA,
            pltpu.SemaphoreType.DMA((span // chunk,)),
            pltpu.SemaphoreType.DMA((n_peers,)),
            pltpu.SemaphoreType.DMA((total,)),
            pltpu.SemaphoreType.DMA,
            pltpu.SemaphoreType.DMA((total,)),
        ],
        compiler_params=pltpu.CompilerParams(
            collective_id=0, has_side_effects=True, vmem_limit_bytes=60 * 1024 * 1024
        ),
        name="search",
    )(
        queries, candidates, shortlist, edges,
        row_scale.reshape(count_rows // LANES, LANES), codes.T, quant_rows,
    )
    return pl.pallas_call(
        finish,
        out_shape=(
            jax.ShapeDtypeStruct((rows_q, edges.shape[0] - 1), f32),
            jax.ShapeDtypeStruct(candidates.shape, f32),
        ),
        in_specs=[spec(memory_space=vmem)],
        out_specs=(spec(memory_space=vmem), spec(memory_space=vmem)),
        name="finish",
    )(rows)


def solution(mesh):
    return jax.shard_map(
        functools.partial(shards, mesh.shape["corpus"], mesh.shape["batch"]),
        mesh=mesh,
        in_specs=(
            P(("corpus", "batch"), None),
            P("corpus", None),
            P("corpus", None),
            P("corpus"),
            P(("corpus", "batch"), None),
            P(("corpus", "batch")),
            P(),
        ),
        out_specs=(P(("corpus", "batch"), None), P(("corpus", "batch"), None)),
        check_vma=False,
    )
```

```python
import functools

import jax
import jax.numpy as jnp
from jax import lax
from jax.experimental import pallas as pl
from jax.experimental.pallas import tpu as pltpu
from jax.sharding import PartitionSpec as P

LANES = 128
HIST_AT = 64


def grid_of(n):
    side = 1
    while 2 * side**3 < n:
        side += 1
    return (n // (side * side), side, side) if 2 * side**3 == n else (n, 1, 1)


def kernel(
    n, cores, queries_hbm, cands_hbm, lens_hbm, edges_hbm, scale_hbm, codes_hbm, quant_hbm,
    out,
    queries, cands, lens, edges, scale, own, gathered, words, quant, plus, flat, split, signs, marks, part, ham_a, ham_b, raw_a, raw_b, part_out, part_in,
    small_sem, words_sem, quant_sem, send_sem, recv_sem, out_sem, in_sem,
):
    zs, ys, xs = grid_of(n)
    chip, core = lax.axis_index("corpus"), lax.axis_index("batch")
    me = chip * cores + core
    rows_q, width = queries.shape
    total = n * cores
    span = quant.shape[0]
    count_k = edges.shape[0]
    chunk = quant.shape[0] // quant_sem.shape[0]
    first = core * span

    z, y, x = chip // (ys * xs), (chip // xs) % ys, chip % xs
    even = core % 2 == 0
    stride_b = jnp.where(even, xs, 1)
    stride_c = jnp.where(even, 1, xs)
    b, c = jnp.where(even, y, x), jnp.where(even, x, y)
    bs, cs = ys, xs

    def chip_at(zz, bb, cc):
        return zz * (ys * xs) + bb * stride_b + cc * stride_c

    barrier = pltpu.get_barrier_semaphore()
    peers = []
    for i in range(1, zs):
        peers.append((chip_at((z + i) % zs, b, c), core))
    for i in range(1, bs):
        peers.append((chip_at(z, (b + i) % bs, c), core))
    for i in range(1, cs):
        peers.append((chip_at(z, b, (c + i) % cs), core))
    for i in range(1, cores):
        peers.append((chip, (core + i) % cores))
    for to in peers:
        pl.semaphore_signal(barrier, inc=1, device_id=to, device_id_type=pl.DeviceIdType.MESH)
    smalls = [
        pltpu.make_async_copy(source, target, small_sem.at[i])
        for i, (source, target) in enumerate(
            (
                (queries_hbm, queries), (cands_hbm, cands), (lens_hbm, lens),
                (edges_hbm, edges), (scale_hbm, scale),
            )
        )
    ]
    for copy in smalls:
        copy.start()

    words_copy = pltpu.make_async_copy(
        codes_hbm.at[:, pl.ds(pl.multiple_of(first, LANES), span)], words, words_sem
    )
    words_copy.start()

    def quant_copy(i):
        at = pl.multiple_of(first + i * chunk, chunk)
        to = pl.multiple_of(i * chunk, chunk)
        return pltpu.make_async_copy(
            quant_hbm.at[pl.ds(at, chunk)], quant.at[pl.ds(to, chunk)], quant_sem.at[i]
        )

    for i in range(quant_sem.shape[0]):
        quant_copy(i).start()

    for copy in smalls:
        copy.wait()

    own[:, :width] = queries[...]
    row = lax.broadcasted_iota(jnp.int32, cands.shape, 0)
    slot = lax.broadcasted_iota(jnp.int32, cands.shape, 1)
    length = jnp.zeros(cands.shape, jnp.int32)
    for i in range(rows_q):
        length = jnp.where(row == i, lens[i], length)
    own[:, width:] = jnp.full((rows_q, LANES), -1.0, jnp.float32)
    own[:, width : width + cands.shape[1]] = jnp.where(
        slot < length, cands[...], -1
    ).astype(jnp.float32)

    pl.semaphore_wait(barrier, len(peers))
    n_peers = len(peers)
    to_z, to_b = zs - 1, bs - 1
    to_c = cs - 1

    def block_copy(block, kind, to, mine=False):
        return pltpu.make_async_remote_copy(
            src_ref=own if mine else gathered.at[block],
            dst_ref=gathered.at[block],
            send_sem=send_sem.at[kind],
            recv_sem=recv_sem.at[block],
            device_id=to,
            device_id_type=pl.DeviceIdType.MESH,
        )

    def got(block):
        pltpu.make_async_copy(gathered.at[block], gathered.at[block], recv_sem.at[block]).wait()

    def pass_on(block, lo, mine=False):
        for kind in range(lo, n_peers):
            block_copy(block, kind, peers[kind], mine).start()

    both_sides = jnp.minimum(z, zs - 1 - z)
    far_side = jnp.where(z < zs - 1 - z, 1, -1)

    def z_at(p):
        near = p <= 2 * both_sides
        away = jnp.where(near, (p + 1) // 2, p - both_sides)
        side = jnp.where(near, 2 * (p % 2) - 1, far_side)
        return z + away * side

    def block_z(p):
        return chip_at(z_at(p), b, c) * cores + core

    def block_b(i):
        return chip_at(z_at(i % zs), (b + 1 + i // zs) % bs, c) * cores + core

    def block_c(i):
        to = (c + 1 + i // (zs * bs)) % cs
        return chip_at(z_at(i % zs), (b + (i // zs) % bs) % bs, to) * cores + core

    def block_d(i):
        return (i % n) * cores + (core + 1 + i // n) % cores

    def sent():
        counts = [1] * to_z + [zs] * to_b + [zs * bs] * to_c + [n] * (cores - 1)
        for kind, count in enumerate(counts):
            some = gathered.at[pl.ds(0, count)]
            pltpu.make_async_copy(some, some, send_sem.at[kind]).wait()

    count_b, count_c, count_d = zs * to_b, zs * bs * to_c, n * (cores - 1)
    at_b, at_c, at_d = to_z, to_z + to_b, to_z + to_b + to_c

    def loop(lo, hi, body):
        def step(i, carry):
            body(i)
            return carry

        lax.fori_loop(lo, hi, step, 0)

    bit = lax.broadcasted_iota(jnp.int32, (32, span // 2), 0)

    def unpack(lo, hi):
        def step(w):
            for half in range(2):
                cols = slice(half * (span // 2), (half + 1) * (span // 2))
                word = jnp.broadcast_to(words[pl.ds(w, 1), cols], bit.shape)
                bits = jnp.bitwise_and(lax.shift_right_logical(word, bit), 1)
                plus[pl.ds(pl.multiple_of(w * 32, 32), 32), cols] = bits.astype(
                    jnp.float32
                ).astype(jnp.float8_e4m3fn)

        loop(lo, hi, step)

    count_w = words.shape[0]
    cut = [count_w * i // 4 for i in range(5)]

    pass_on(me, 0, True)
    gathered[me] = own[...]
    words_copy.wait()
    unpack(cut[0], cut[1])

    def relay(block_of, lo, start=0):
        def step(i):
            block = block_of(i)
            got(block)
            pass_on(block, lo)

        return step

    loop(1, min(2, zs), relay(block_z, at_b))
    loop(0, to_b, lambda i: relay(block_b, at_c)(i * zs))
    loop(min(2, zs), zs, relay(block_z, at_b))
    unpack(cut[1], cut[2])
    loop(0, to_b * (zs - 1), lambda i: relay(block_b, at_c)(i // (zs - 1) * zs + 1 + i % (zs - 1)))
    unpack(cut[2], cut[3])
    loop(0, count_c, relay(block_c, at_d))
    unpack(cut[3], cut[4])
    loop(0, count_d, lambda i: got(block_d(i)))

    def lay(i):
        pair = jnp.concatenate([gathered[2 * i], gathered[2 * i + 1]], axis=0)
        flat[pl.ds(pl.multiple_of(i * 2 * rows_q, 2 * rows_q), 2 * rows_q), :] = pair

    loop(0, total // 2, lay)
    for i in range(quant_sem.shape[0]):
        quant_copy(i).wait()

    tile_q = marks.shape[1]
    unit = ham_a.shape[1]
    groups = span // unit
    base = (chip * cores + core) * span
    limits = [(edges[k] - width // 2).astype(jnp.float32).astype(jnp.bfloat16) for k in range(count_k)]

    def tile(t):
        q_at = pl.multiple_of(t * tile_q, tile_q)
        vecs = flat[pl.ds(q_at, tile_q), :width]
        index = flat[pl.ds(q_at, tile_q), width:].astype(jnp.int32) - base
        high = vecs.astype(jnp.bfloat16)
        split[:tile_q] = high
        split[tile_q:] = (vecs - high.astype(jnp.float32)).astype(jnp.bfloat16)
        sign = jnp.where(vecs >= 0, 1.0, -1.0)
        signs[...] = sign.astype(jnp.float8_e4m3fn)
        half_sum = jnp.sum(sign, axis=1, keepdims=True) * 0.5
        lane = jnp.bitwise_and(index, LANES - 1)
        where = lax.shift_right_arithmetic(index, 7)
        marks[...] = jnp.zeros_like(marks)
        part[...] = jnp.zeros_like(part)

        def multiply(g, ham, raw):
            r_at = pl.multiple_of(g * unit, unit)
            dots = jnp.dot(signs[...], plus[:, pl.ds(r_at, unit)], preferred_element_type=jnp.float32)
            ham[...] = (half_sum - dots).astype(jnp.bfloat16)
            both = lax.dot_general(
                split[...], quant[pl.ds(r_at, unit), :], (((1,), (1,)), ((), ())),
                preferred_element_type=jnp.float32,
            )
            raw[...] = both[:tile_q] + both[tile_q:]

        def collect(g, ham, raw):
            one = jnp.ones((tile_q, LANES), jnp.bfloat16)
            for k in range(count_k):
                mark = marks[k]
                for j in range(unit // LANES):
                    piece = ham[:, j * LANES : (j + 1) * LANES]
                    mark = mark + jnp.where(piece >= limits[k], one, jnp.zeros_like(one))
                marks[k] = mark
            score = part[...]
            for j in range(unit // LANES):
                row_at = core * (span // LANES) + g * (unit // LANES) + j
                piece = raw[:, j * LANES : (j + 1) * LANES] * scale[pl.ds(row_at, 1), :]
                picked = jnp.take_along_axis(piece, lane, axis=1, mode="promise_in_bounds")
                score = jnp.where(where == g * (unit // LANES) + j, picked, score)
            part[...] = score

        def step(p):
            multiply(2 * p + 1, ham_b, raw_b)
            collect(2 * p, ham_a, raw_a)
            multiply(2 * p + 2, ham_a, raw_a)
            collect(2 * p + 1, ham_b, raw_b)

        multiply(0, ham_a, raw_a)
        loop(0, groups // 2 - 1, step)
        multiply(groups - 1, ham_b, raw_b)
        collect(groups - 2, ham_a, raw_a)
        collect(groups - 1, ham_b, raw_b)
        columns = lax.broadcasted_iota(jnp.int32, (LANES, LANES), 1)
        result = part[...]
        for k in range(count_k):
            spot = jnp.where(columns == HIST_AT + k, 1.0, 0.0).astype(jnp.bfloat16)
            result = result + jnp.dot(marks[k], spot, preferred_element_type=jnp.float32)
        per = tile_q // rows_q
        for i in range(per):
            part_out[t * per + i] = result[i * rows_q : (i + 1) * rows_q]

    loop(0, flat.shape[0] // tile_q, tile)

    def result_copy(i):
        to = (me + i) % total
        return pltpu.make_async_remote_copy(
            src_ref=part_out.at[to],
            dst_ref=part_in.at[me],
            send_sem=out_sem,
            recv_sem=in_sem.at[me],
            device_id=(to // cores, to % cores),
            device_id_type=pl.DeviceIdType.MESH,
        )

    loop(1, total, lambda i: result_copy(i).start())
    part_in[me] = part_out[me]

    def wait_in(i):
        source = (me + i) % total
        pltpu.make_async_copy(part_in.at[source], part_in.at[source], in_sem.at[source]).wait()

    loop(1, total, wait_in)
    summed = jnp.sum(part_in[...], axis=0)
    bins = count_k - 1
    above = summed[:, HIST_AT : HIST_AT + bins] - summed[:, HIST_AT + 1 : HIST_AT + 1 + bins]
    out[:, HIST_AT : HIST_AT + bins] = above * (bins / (total * span))
    out[:, : cands.shape[1]] = summed[:, : cands.shape[1]]

    rest = part_in.at[pl.ds(0, total - 1)]
    pltpu.make_async_copy(rest, rest, out_sem).wait()
    sent()


def finish(rows, hist, scores):
    hist[...] = rows[:, HIST_AT : HIST_AT + hist.shape[1]]
    scores[...] = rows[:, : scores.shape[1]]


def shards(n, cores, queries, codes, quant_rows, row_scale, candidates, shortlist, edges):
    rows_q, width = queries.shape
    count_rows, count_w = codes.shape
    span = count_rows // cores
    total = n * cores
    tile_q = 128
    chunk = 512
    unit = 512
    vmem, smem, hbm = pltpu.VMEM, pltpu.SMEM, pl.ANY
    zs, ys, xs = grid_of(n)
    n_peers = zs + ys + xs + cores - 4
    f32, bf16 = jnp.float32, jnp.bfloat16
    spec = pl.BlockSpec
    rows = pl.pallas_call(
        functools.partial(kernel, n, cores),
        out_shape=jax.ShapeDtypeStruct((rows_q, LANES), f32),
        in_specs=[
            spec(memory_space=hbm) for _ in range(7)
        ],
        out_specs=spec(memory_space=vmem),
        scratch_shapes=[
            vmem(queries.shape, f32),
            vmem(candidates.shape, jnp.int32),
            smem(shortlist.shape, jnp.int32),
            smem(edges.shape, jnp.int32),
            vmem((count_rows // LANES, LANES), f32),
            vmem((rows_q, width + LANES), f32),
            vmem((total, rows_q, width + LANES), f32),
            vmem((count_w, span), jnp.int32),
            vmem((span, width), bf16),
            vmem((width, span), jnp.float8_e4m3fn),
            vmem((total * rows_q, width + LANES), f32),
            vmem((2 * tile_q, width), bf16),
            vmem((tile_q, width), jnp.float8_e4m3fn),
            vmem((edges.shape[0], tile_q, LANES), bf16),
            vmem((tile_q, LANES), f32),
            vmem((tile_q, unit), bf16),
            vmem((tile_q, unit), bf16),
            vmem((tile_q, unit), f32),
            vmem((tile_q, unit), f32),
            vmem((total, rows_q, LANES), f32),
            vmem((total, rows_q, LANES), f32),
            pltpu.SemaphoreType.DMA((5,)),
            pltpu.SemaphoreType.DMA,
            pltpu.SemaphoreType.DMA((span // chunk,)),
            pltpu.SemaphoreType.DMA((n_peers,)),
            pltpu.SemaphoreType.DMA((total,)),
            pltpu.SemaphoreType.DMA,
            pltpu.SemaphoreType.DMA((total,)),
        ],
        compiler_params=pltpu.CompilerParams(
            collective_id=0, has_side_effects=True, vmem_limit_bytes=60 * 1024 * 1024
        ),
        name="search",
    )(
        queries, candidates, shortlist, edges,
        row_scale.reshape(count_rows // LANES, LANES), codes.T, quant_rows,
    )
    return pl.pallas_call(
        finish,
        out_shape=(
            jax.ShapeDtypeStruct((rows_q, edges.shape[0] - 1), f32),
            jax.ShapeDtypeStruct(candidates.shape, f32),
        ),
        in_specs=[spec(memory_space=vmem)],
        out_specs=(spec(memory_space=vmem), spec(memory_space=vmem)),
        name="finish",
    )(rows)


def solution(mesh):
    return jax.shard_map(
        functools.partial(shards, mesh.shape["corpus"], mesh.shape["batch"]),
        mesh=mesh,
        in_specs=(
            P(("corpus", "batch"), None),
            P("corpus", None),
            P("corpus", None),
            P("corpus"),
            P(("corpus", "batch"), None),
            P(("corpus", "batch")),
            P(),
        ),
        out_specs=(P(("corpus", "batch"), None), P(("corpus", "batch"), None)),
        check_vma=False,
    )
```
